128 devices in a mesh: tm: 32 (over y, x, core), obj: 4 (over z).
Axes of the slice: x: 4, y: 4, z: 4, core: 2. Of those that a mesh axis runs over, the one named last changes fastest.
Arguments:
- objective: float32 [128, 768, 768], P('tm', 'obj'), parts along dimension 1, may hold values from -6 to 6
- jacobians: bfloat16 [128, 768, 768], P('tm'), may hold values from -0.21875 to 0.21875
- precond_blocks: bfloat16 [2, 128, 768, 768], P(None, 'tm'), as said below
Outputs:
- adjoint: float32 [128, 768, 768], P('tm', 'obj'), parts along dimension 1
- residual: float32 [128, 768, 768], P('tm', 'obj'), parts along dimension 1
The draws below stay inside these ranges and needn't reach their ends.
There are 4 independent parts, one for each index of `obj`. The reference program is written for one: setup_inputs(seed, part) draws one part's arguments, and reference() takes and returns one part's arrays. A program takes and returns all parts, laid end to end along the dimension named above; an argument that names none is the same for every part. Nothing has to cross between parts.
Inputs may be any that keep to these rules, and one draw needn't show every extreme that they name: precond_blocks[0, j] equals precond_blocks[0, (128 - j) mod 128] and precond_blocks[1, j] equals - precond_blocks[1, (128 - j) mod 128].
All inputs are finite; a program needn't handle non-finite values.
Results may differ from the reference program's by a relative error of at most 0.0087.
Values may be sent and summed in bfloat16 or wider, within the bound.
No kernel may reach another device: no remote copies, remote signals or barrier semaphores. Data moves between devices by JAX's collectives and lax.ppermute only.
A program may use at most 128 MiB of HBM per device.

```python
import math
import jax
import jax.numpy as jnp
from jax import lax

NS = 768
COLS = 192
ITERS = 2
STEPS = 128


def draw_precond_blocks(key, part):
    first_key, second_key = jax.random.split(jax.random.fold_in(key, 17))
    block_shape = (STEPS, NS, NS)
    real_noise = jax.random.normal(first_key, block_shape, jnp.float32)
    imag_noise = jax.random.normal(second_key, block_shape, jnp.float32)
    mirror = (STEPS - jnp.arange(STEPS)) % STEPS
    spread = 0.8 / math.sqrt(NS)
    real_part = 0.5 * (real_noise + real_noise[mirror]) * spread + jnp.eye(NS, dtype=jnp.float32)[None]
    imag_part = 0.5 * (imag_noise - imag_noise[mirror]) * spread
    return jnp.stack([real_part, imag_part]).astype(jnp.bfloat16)


def shard_levels(rng, shape, cuts, least, top_value):
    level, own = 1.0, jax.random.fold_in(rng, 6)
    for position, shards_of in cuts:
        heights = jnp.exp(jax.random.uniform(jax.random.fold_in(own, position), (shards_of,), jnp.float32, least / len(cuts), top_value / len(cuts)))
        level = level * jnp.repeat(heights, shape[position] // shards_of).reshape([-1 if axis == position else 1 for axis in range(len(shape))])
    return level


def centred(own_key, extent, scale, reach, cuts=(), kind=jnp.bfloat16):
    array = scale * jax.random.normal(own_key, extent, jnp.float32)
    if cuts:
        array = array * shard_levels(own_key, extent, cuts, -0.22, 0.18)
    return jnp.clip(array, -reach, reach).astype(kind)


def setup_inputs(seed: int = 0, part: int = 0) -> dict:
    key_of = jax.random.split(jax.random.key(seed), 4)
    part_keys = jax.random.split(jax.random.fold_in(key_of[3], part), 4)
    return {
        "objective": centred(part_keys[0], (STEPS, COLS, NS), 1.0, 6.0, ((0, 32),), jnp.float32),
        "jacobians": centred(key_of[1], (STEPS, NS, NS), NS ** -0.5, 0.21875, ((0, 32),)),
        "precond_blocks": draw_precond_blocks(jax.random.fold_in(key_of[3], 71), part),
    }


log_alpha = math.log(0.05)


def tables(count):
    indices = jnp.arange(count, dtype=jnp.int32)
    product = (indices[:, None] * indices[None, :]) % count
    angles = product.astype(jnp.float32) * (2.0 * math.pi / count)
    return jnp.cos(angles), jnp.sin(angles)


def frequency_product(operands):
    spectrum_real, spectrum_imag, block_real, block_imag = operands
    zeta_real = spectrum_real.astype(jnp.float32)
    zeta_imag = spectrum_imag.astype(jnp.float32)
    matrix_real = block_real.astype(jnp.float32)
    matrix_imag = block_imag.astype(jnp.float32)
    highest = lax.Precision.HIGHEST
    wave_real = jnp.dot(zeta_real, matrix_real, precision=highest) - jnp.dot(zeta_imag, matrix_imag, precision=highest)
    wave_imag = jnp.dot(zeta_real, matrix_imag, precision=highest) + jnp.dot(zeta_imag, matrix_real, precision=highest)
    return wave_real.astype(jnp.bfloat16), wave_imag.astype(jnp.bfloat16)


def precondition(residual, precond_blocks):
    highest = lax.Precision.HIGHEST
    positions = jnp.arange(STEPS, dtype=jnp.float32)
    forward_scale = jnp.exp(positions * (-log_alpha / STEPS))
    inverse_factor = jnp.exp(positions * (log_alpha / STEPS)) / STEPS
    cosine_table, sine_table = tables(STEPS)
    scaled = residual * forward_scale[:, None, None]
    flattened = scaled.reshape(STEPS, -1)
    spectrum_real = jnp.dot(cosine_table, flattened, precision=highest).astype(jnp.bfloat16)
    spectrum_imag = (-jnp.dot(sine_table, flattened, precision=highest)).astype(jnp.bfloat16)
    spectrum_real = spectrum_real.reshape(STEPS, COLS, NS)
    spectrum_imag = spectrum_imag.reshape(STEPS, COLS, NS)
    wave_real, wave_imag = lax.map(frequency_product, (spectrum_real, spectrum_imag, precond_blocks[0], precond_blocks[1]))
    real_flat = wave_real.astype(jnp.float32).reshape(STEPS, -1)
    imag_flat = wave_imag.astype(jnp.float32).reshape(STEPS, -1)
    values = (jnp.dot(cosine_table, real_flat, precision=highest) - jnp.dot(sine_table, imag_flat, precision=highest)) * inverse_factor[:, None]
    return values.reshape(STEPS, COLS, NS)


def apply_operator(correction, jacobians):
    following = jnp.concatenate([correction[1:], jnp.zeros_like(correction[:1])], axis=0).astype(jnp.bfloat16)
    carried = jnp.einsum("kcn,knm->kcm", following.astype(jnp.float32), jacobians.astype(jnp.float32), precision=lax.Precision.HIGHEST)
    return correction - carried


def reference(objective, jacobians, precond_blocks):
    adjoint = jnp.zeros_like(objective)
    residual = objective
    for iteration in range(ITERS):
        correction = precondition(residual, precond_blocks)
        adjoint = adjoint + correction
        residual = residual - apply_operator(correction, jacobians)
    return adjoint, residual
```

```python
import math

import jax
import jax.numpy as jnp
import numpy as np
from jax import lax
from jax.sharding import PartitionSpec as P

ITERS = 2
log_alpha = math.log(0.05)


def split_table(table):
    high = table.astype(jnp.bfloat16)
    low = (table - high.astype(np.float64)).astype(jnp.bfloat16)
    return high, low


def tables(steps, groups):
    times = np.arange(steps)
    forward = np.zeros((2, groups, 4, 2, steps))
    backward = np.zeros((2, steps, 2, groups, 4))
    grow = np.exp(times * (-log_alpha / steps))
    shrink = np.exp(times * (log_alpha / steps)) / steps
    for group in range(groups):
        low_side = group < groups // 2
        for position in range(2):
            first = (0 if low_side else 1) ^ position
            jobs = [(0, 4 * group + 1, position), (2, 4 * group + 2 * position, first)]
            for slot, frequency, half in jobs:
                angle = 2.0 * math.pi * ((frequency * times) % steps) / steps
                cosine, sine = np.cos(angle), np.sin(angle)
                if frequency % (steps // 2) == 0:
                    for at, part in ((slot, half), (slot + 1, 1 - half)):
                        forward[position, group, at, part] = cosine * grow
                        backward[part, :, position, group, at] = cosine * shrink
                    continue
                forward[position, group, slot, half] = cosine * grow
                forward[position, group, slot + 1, half] = -sine * grow
                backward[half, :, position, group, slot] = 2.0 * cosine * shrink
                backward[half, :, position, group, slot + 1] = -2.0 * sine * shrink
    size = 2 * steps
    return forward.reshape(size, size), backward.reshape(size, size)


def exchange(block):
    return lax.all_to_all(block, "tm", split_axis=0, concat_axis=0, tiled=True)


def transform(pair, rows):
    high, low = pair
    return jnp.dot(high, rows, preferred_element_type=jnp.float32) + jnp.dot(
        low, rows, preferred_element_type=jnp.float32
    )


def mul(left, right):
    return jnp.dot(left, right, preferred_element_type=jnp.float32)


def body(objective, jacobians, precond_blocks):
    local_steps, columns, states = objective.shape
    groups = lax.axis_size("tm")
    steps = local_steps * groups
    per_piece = columns // groups
    third = per_piece // 2
    forward, backward = tables(steps, groups)
    forward, backward = split_table(forward), split_table(backward)
    real, imag = precond_blocks[0], precond_blocks[1]
    route = [(i + 1, i) for i in range(groups - 1)]
    adjoint = None
    residual = objective
    for _ in range(ITERS):
        send = residual.astype(jnp.bfloat16).transpose(1, 0, 2)
        pieces = exchange(send).reshape(groups, 2, third, local_steps, states)
        rows = pieces.transpose(1, 0, 3, 2, 4).reshape(2 * steps, third * states)
        spectrum = transform(forward, rows).astype(jnp.bfloat16)
        spectrum = spectrum.reshape(2, groups, 4, third, states).transpose(1, 0, 3, 2, 4)
        spectrum = exchange(spectrum.reshape(columns, 4, states))
        spectrum = spectrum.reshape(groups, 2, third, 4, states).transpose(3, 1, 0, 2, 4)
        wave = []
        one_re = spectrum[0].reshape(columns, states)
        one_im = spectrum[1].reshape(columns, states)
        w_re = mul(one_re, real[1]) - mul(one_im, imag[1])
        w_im = mul(one_re, imag[1]) + mul(one_im, real[1])
        shape = (1, 2, groups, third, states)
        wave += [w_re.astype(jnp.bfloat16).reshape(shape), w_im.astype(jnp.bfloat16).reshape(shape)]
        other = [[], []]
        for position in range(2):
            x_re = spectrum[2, position].reshape(columns // 2, states)
            x_im = spectrum[3, position].reshape(columns // 2, states)
            b_re, b_im = real[2 * position], imag[2 * position]
            other[0].append((mul(x_re, b_re) - mul(x_im, b_im)).astype(jnp.bfloat16))
            other[1].append((mul(x_re, b_im) + mul(x_im, b_re)).astype(jnp.bfloat16))
        wave += [jnp.stack(part).reshape(shape) for part in other]
        wave = jnp.concatenate(wave, axis=0).transpose(2, 1, 3, 0, 4)
        wave = exchange(wave.reshape(columns, 4, states))
        rows = wave.reshape(groups, 2, third, 4, states).transpose(1, 0, 3, 2, 4)
        values = transform(backward, rows.reshape(2 * steps, third * states))
        values = values.astype(jnp.bfloat16).reshape(2, groups, local_steps, third, states)
        values = values.transpose(1, 0, 3, 2, 4).reshape(columns, local_steps, states)
        correction = exchange(values).transpose(1, 0, 2)
        next_row = lax.ppermute(correction[:1], "tm", route)
        following = jnp.concatenate([correction[1:], next_row], axis=0)
        carried = jnp.einsum(
            "kcn,knm->kcm", following, jacobians, preferred_element_type=jnp.float32
        )
        correction = correction.astype(jnp.float32)
        adjoint = correction if adjoint is None else adjoint + correction
        residual = residual - (correction - carried)
    return (adjoint, residual)


def solution(mesh):
    in_specs = (P("tm", "obj", None), P("tm", None, None), P(None, "tm", None, None))
    out_specs = (P("tm", "obj", None), P("tm", "obj", None))
    return jax.shard_map(body, mesh=mesh, in_specs=in_specs, out_specs=out_specs, check_vma=False)
```

```python
import functools
import math

import jax
import jax.numpy as jnp
import numpy as np
from jax import lax
from jax.experimental import pallas as pl
from jax.experimental.pallas import tpu as pltpu
from jax.sharding import PartitionSpec as P

ITERS = 2
log_alpha = math.log(0.05)
MIB = 1 << 20


def split_table(table):
    high = table.astype(jnp.bfloat16)
    low = (table - high.astype(np.float64)).astype(jnp.bfloat16)
    return np.concatenate([high, low], axis=1)


def tables(steps, groups):
    local = steps // groups
    times = np.arange(steps)
    forward = np.zeros((groups, 2, 4, 2, steps))
    backward = np.zeros((2, steps, groups, 2, 4))
    grow = np.exp(times * (-log_alpha / steps))
    shrink = np.exp(times * (log_alpha / steps)) / steps
    for group in range(groups):
        low_side = group < groups // 2
        for position in range(2):
            first = (0 if low_side else 1) ^ position
            jobs = [(0, 4 * group + 1, position), (2, 4 * group + 2 * position, first)]
            for slot, frequency, half in jobs:
                angle = 2.0 * math.pi * ((frequency * times) % steps) / steps
                cosine, sine = np.cos(angle), np.sin(angle)
                if frequency % (steps // 2) == 0:
                    for at, part in ((slot, half), (slot + 1, 1 - half)):
                        forward[group, position, at, part] = cosine * grow
                        backward[part, :, group, position, at] = cosine * shrink
                    continue
                forward[group, position, slot, half] = cosine * grow
                forward[group, position, slot + 1, half] = -sine * grow
                backward[half, :, group, position, slot] = 2.0 * cosine * shrink
                backward[half, :, group, position, slot + 1] = -2.0 * sine * shrink
    size = 2 * steps
    forward = forward.reshape(size, 2, groups, local).transpose(0, 2, 1, 3)
    backward = backward.reshape(2, groups, local, size).transpose(1, 0, 2, 3)
    return forward.reshape(size, size), backward.reshape(size, size)


def shuffles(groups):
    size = 8 * groups
    pack = np.zeros((groups, 2, 4, 4, 2, groups))
    sort = np.zeros((4, 2, groups, groups, 2, 4))
    for piece in range(groups):
        for half in range(2):
            for step in range(4):
                pack[piece, half, step, step, half, piece] = 1
                sort[step, half, piece, piece, half, step] = 1
    shape = (size, size)
    return pack.reshape(shape).astype(jnp.bfloat16), sort.reshape(shape).astype(jnp.bfloat16)


def mul(left, right):
    return jnp.dot(left, right, preferred_element_type=jnp.float32)


def rows_of(ref, third):
    groups, _, eight, states = ref.shape
    wide = ref[:, third].astype(jnp.float32)
    return wide.reshape(groups * eight, states).astype(jnp.bfloat16)


def put_rows(ref, third, rows):
    groups, _, eight, states = ref.shape
    ref[:, third] = rows.reshape(groups, eight, states).astype(ref.dtype)


def pack_kernel(block_ref, pack_ref, send_ref):
    steps, columns, states = block_ref.shape
    rows = block_ref[...].reshape(steps * columns, states).astype(jnp.bfloat16)
    put_rows(send_ref, 0, mul(pack_ref[...], rows))


def transform_kernel(in_ref, table_ref, out_ref):
    for third in range(in_ref.shape[1]):
        rows = rows_of(in_ref, third)
        put_rows(out_ref, third, mul(table_ref[...], jnp.concatenate([rows, rows], axis=0)))


def multiply_kernel(in_ref, sort_ref, unsort_ref, blocks_ref, out_ref, held, sorted_ref, sem):
    groups, thirds, _, states = in_ref.shape
    copies = []
    for index, frequency in enumerate((1, 0, 2)):
        for part in range(2):
            copies.append(
                pltpu.make_async_copy(
                    blocks_ref.at[part, frequency], held.at[index, part], sem.at[index, part]
                )
            )
            copies[-1].start()
    half = thirds * groups
    for third in range(thirds):
        rows = mul(sort_ref[...], rows_of(in_ref, third)).astype(jnp.bfloat16)
        for block in range(8):
            at = block * half + third * groups
            sorted_ref[at : at + groups] = rows[block * groups : (block + 1) * groups]
    for copy in copies[:2]:
        copy.wait()

    def product(index, rows, length):
        left = sorted_ref[rows : rows + length]
        count = length // 2
        y = mul(left, held[index, 0])
        z = mul(left, held[index, 1])
        sorted_ref[rows : rows + count] = (y[:count] - z[count:]).astype(jnp.bfloat16)
        sorted_ref[rows + count : rows + length] = (z[:count] + y[count:]).astype(jnp.bfloat16)

    def pair_product(index, re_at, im_at):
        left = jnp.concatenate(
            [sorted_ref[re_at : re_at + half], sorted_ref[im_at : im_at + half]], axis=0
        )
        y = mul(left, held[index, 0])
        z = mul(left, held[index, 1])
        sorted_ref[re_at : re_at + half] = (y[:half] - z[half:]).astype(jnp.bfloat16)
        sorted_ref[im_at : im_at + half] = (z[:half] + y[half:]).astype(jnp.bfloat16)

    product(0, 0, 4 * half)
    for index in (1, 2):
        for copy in copies[2 * index : 2 * index + 2]:
            copy.wait()
        pair_product(index, (4 + index - 1) * half, (6 + index - 1) * half)
    for third in range(thirds):
        at = third * groups
        rows = [sorted_ref[block * half + at : block * half + at + groups] for block in range(8)]
        put_rows(out_ref, third, mul(unsort_ref[...], jnp.concatenate(rows, axis=0)))


def unpack_kernel(in_ref, unpack_ref, first_ref, out_ref):
    steps, columns, states = out_ref.shape
    width = columns // in_ref.shape[1]
    for third in range(in_ref.shape[1]):
        rows = mul(unpack_ref[...], rows_of(in_ref, third)).astype(jnp.bfloat16)
        rows = rows.reshape(steps, width, states)
        out_ref[:, third * width : (third + 1) * width] = rows
        first_ref[third * width : (third + 1) * width] = rows[0]


def update_kernel(last, correction_ref, before_ref, next_ref, residual_ref, jacobians_ref,
                  pack_ref, out_ref, extra_ref, held, sem):
    steps, columns, states = correction_ref.shape
    copies = [
        pltpu.make_async_copy(jacobians_ref.at[step], held.at[step], sem.at[step])
        for step in range(steps)
    ]
    for copy in copies:
        copy.start()
    for step in range(steps):
        correction = correction_ref[step].astype(jnp.float32)
        if last:
            extra_ref[step] = before_ref[step].astype(jnp.float32) + correction
        following = correction_ref[step + 1] if step + 1 < steps else next_ref[...]
        copies[step].wait()
        carried = mul(following, held[step])
        out_ref[step] = residual_ref[step] - (correction - carried)
    if not last:
        thirds = extra_ref.shape[1]
        width = columns // thirds
        for third in range(thirds):
            rows = out_ref[:, third * width : (third + 1) * width].astype(jnp.bfloat16)
            put_rows(extra_ref, third, mul(pack_ref[...], rows.reshape(steps * width, states)))


def vmem():
    return pl.BlockSpec(memory_space=pltpu.VMEM)


def call(kernel, out_shape, args, limit, scratch=(), hbm=(), flops=1 << 28, **kwargs):
    return pl.pallas_call(
        kernel,
        out_shape=out_shape,
        in_specs=[
            pl.BlockSpec(memory_space=pl.ANY) if i in hbm else vmem() for i in range(len(args))
        ],
        out_specs=jax.tree.map(lambda _: vmem(), out_shape),
        scratch_shapes=list(scratch),
        compiler_params=pltpu.CompilerParams(vmem_limit_bytes=limit * MIB),
        cost_estimate=pl.CostEstimate(flops=flops, bytes_accessed=4 * MIB, transcendentals=0),
        **kwargs,
    )(*args)


def exchange(block):
    return lax.all_to_all(block, "tm", split_axis=0, concat_axis=0, tiled=True)


def body(objective, jacobians, precond_blocks):
    local_steps, columns, states = objective.shape
    groups = lax.axis_size("tm")
    steps = local_steps * groups
    thirds = columns // (2 * groups)
    width = columns // thirds
    forward, backward = (jnp.asarray(split_table(t)) for t in tables(steps, groups))
    pack, sort = shuffles(groups)
    unpack, unsort = jnp.asarray(pack.T.copy()), jnp.asarray(sort.T.copy())
    pack, sort = jnp.asarray(pack), jnp.asarray(sort)
    route = [(i + 1, i) for i in range(groups - 1)]
    wire = jax.ShapeDtypeStruct((groups, thirds, 8, states), jnp.bfloat16)
    field = jax.ShapeDtypeStruct(objective.shape, jnp.float32)
    plain = jax.ShapeDtypeStruct(objective.shape, jnp.bfloat16)
    row = jax.ShapeDtypeStruct((columns, states), jnp.bfloat16)

    send = pl.pallas_call(
        pack_kernel,
        grid=(thirds,),
        out_shape=wire,
        in_specs=[
            pl.BlockSpec((local_steps, width, states), lambda i: (0, i, 0)),
            pl.BlockSpec((2 * steps, 2 * steps), lambda i: (0, 0)),
        ],
        out_specs=pl.BlockSpec((groups, 1, 8, states), lambda i: (0, i, 0, 0)),
        compiler_params=pltpu.CompilerParams(vmem_limit_bytes=16 * MIB),
    )(objective, pack)
    residual = objective
    before = None
    for iteration in range(ITERS):
        last = iteration == ITERS - 1
        rows = call(transform_kernel, wire, (exchange(send), forward), 16)
        rows = call(
            multiply_kernel,
            wire,
            (exchange(rows), sort, unsort, precond_blocks),
            32,
            scratch=[
                pltpu.VMEM((3, 2, states, states), jnp.bfloat16),
                pltpu.VMEM((4 * columns, states), jnp.bfloat16),
                pltpu.SemaphoreType.DMA((3, 2)),
            ],
            hbm=(3,),
            flops=1 << 31,
        )
        rows = call(transform_kernel, wire, (exchange(rows), backward), 16)
        first, correction = call(unpack_kernel, (row, plain), (exchange(rows), unpack), 16)
        following = lax.ppermute(first, "tm", route)
        before = correction if before is None else before
        residual, send = call(
            functools.partial(update_kernel, last),
            (field, field if last else wire),
            (correction, before, following, residual, jacobians, pack),
            32,
            scratch=[
                pltpu.VMEM((local_steps, states, states), jnp.bfloat16),
                pltpu.SemaphoreType.DMA((local_steps,)),
            ],
            hbm=(4,),
            flops=1 << 30,
        )
    return (send, residual)


def solution(mesh):
    in_specs = (P("tm", "obj", None), P("tm", None, None), P(None, "tm", None, None))
    out_specs = (P("tm", "obj", None), P("tm", "obj", None))
    return jax.shard_map(body, mesh=mesh, in_specs=in_specs, out_specs=out_specs, check_vma=False)
```

```python
import math

import jax
import jax.numpy as jnp
import numpy as np
from jax import lax
from jax.experimental import pallas as pl
from jax.experimental.pallas import tpu as pltpu
from jax.sharding import PartitionSpec as P

log_alpha = math.log(0.05)
MIB = 1 << 20
PACK_LIMIT = 16
PRODUCT_LIMIT = 16


def split_table(table):
    high = table.astype(jnp.bfloat16)
    low = (table - high.astype(np.float64)).astype(jnp.bfloat16)
    return np.concatenate([high, low], axis=1)


def tables(steps, groups):
    local = steps // groups
    times = np.arange(steps)
    forward = np.zeros((groups, 2, 4, 2, steps))
    backward = np.zeros((2, steps, groups, 2, 4))
    grow = np.exp(times * (-log_alpha / steps))
    shrink = np.exp(times * (log_alpha / steps)) / steps
    for group in range(groups):
        low_side = group < groups // 2
        for position in range(2):
            first = (0 if low_side else 1) ^ position
            jobs = [(0, 4 * group + 1, position), (2, 4 * group + 2 * position, first)]
            for slot, frequency, half in jobs:
                angle = 2.0 * math.pi * ((frequency * times) % steps) / steps
                cosine, sine = np.cos(angle), np.sin(angle)
                if frequency % (steps // 2) == 0:
                    for at, part in ((slot, half), (slot + 1, 1 - half)):
                        forward[group, position, at, part] = cosine * grow
                        backward[part, :, group, position, at] = cosine * shrink
                    continue
                forward[group, position, slot, half] = cosine * grow
                forward[group, position, slot + 1, half] = -sine * grow
                backward[half, :, group, position, slot] = 2.0 * cosine * shrink
                backward[half, :, group, position, slot + 1] = -2.0 * sine * shrink
    size = 2 * steps
    forward = forward.reshape(size, 2, steps)
    backward = backward.reshape(2, steps, size)

    def by_owner(shift):
        ahead = np.roll(forward, -shift, axis=2).reshape(size, 2, groups, local)
        back = np.roll(backward, -shift, axis=1).reshape(2, groups, local, size)
        ahead = ahead.transpose(0, 2, 1, 3).reshape(size, size)
        return ahead, back.transpose(1, 0, 2, 3).reshape(size, size)

    beyond = np.concatenate([backward[:, local::local], np.zeros((2, 1, size))], axis=1)
    return (*by_owner(0), *by_owner(1), beyond.reshape(2 * groups, size))


def shuffles(groups):
    size = 8 * groups
    pack = np.zeros((groups, 2, 4, 4, 2, groups))
    sort = np.zeros((4, 2, groups, groups, 2, 4))
    for piece in range(groups):
        for half in range(2):
            for step in range(4):
                pack[piece, half, step, step, half, piece] = 1
                sort[step, half, piece, piece, half, step] = 1
    shape = (size, size)
    return pack.reshape(shape).astype(jnp.bfloat16), sort.reshape(shape).astype(jnp.bfloat16)


def mul(left, right):
    return jnp.dot(left, right, preferred_element_type=jnp.float32)


def rows_of(ref, third):
    groups, _, eight, states = ref.shape
    wide = ref[:, third].astype(jnp.float32)
    return wide.reshape(groups * eight, states).astype(jnp.bfloat16)


def put_rows(ref, third, rows):
    groups, _, eight, states = ref.shape
    ref[:, third] = rows.reshape(groups, eight, states).astype(ref.dtype)


def pack_kernel(block_ref, pack_ref, table_ref, send_ref, kept_ref):
    steps, columns, states = block_ref.shape
    rows = block_ref[...].reshape(steps * columns, states).astype(jnp.bfloat16)
    put_rows(send_ref, 0, mul(pack_ref[...], rows))

    @pl.when(pl.program_id(0) == 0)
    def _():
        kept_ref[...] = table_ref[...]


def transform_kernel(*refs):
    *in_refs, table_ref, out_ref = refs
    for third in range(out_ref.shape[1]):
        rows = []
        for in_ref in in_refs:
            rows += [rows_of(in_ref, third)] * 2
        put_rows(out_ref, third, mul(table_ref[...], jnp.concatenate(rows, axis=0)))


def last_transform_kernel(before_ref, in_ref, table_ref, beyond_ref, spread_ref, out_ref):
    groups, thirds = in_ref.shape[:2]
    extra = []
    for third in range(thirds):
        rows = rows_of(in_ref, third)
        rows = jnp.concatenate([rows, rows], axis=0)
        extra.append(mul(beyond_ref[...], rows).astype(jnp.bfloat16))
        before = rows_of(before_ref, third)
        rows = jnp.concatenate([before, before, rows], axis=0)
        put_rows(out_ref, third, mul(table_ref[...], rows))
    extra.append(jnp.zeros_like(extra[0]))
    put_rows(out_ref, thirds, mul(spread_ref[...], jnp.concatenate(extra, axis=0)))


def multiply_kernel(in_ref, sort_ref, unsort_ref, blocks_ref, out_ref, sorted_ref):
    groups, thirds, _, states = in_ref.shape
    half = thirds * groups
    for third in range(thirds):
        rows = mul(sort_ref[...], rows_of(in_ref, third)).astype(jnp.bfloat16)
        for block in range(8):
            at = block * half + third * groups
            sorted_ref[at : at + groups] = rows[block * groups : (block + 1) * groups]

    def product(frequency, re_at, im_at, count):
        left = jnp.concatenate(
            [sorted_ref[re_at : re_at + count], sorted_ref[im_at : im_at + count]], axis=0
        )
        y = mul(left, blocks_ref[0, frequency])
        z = mul(left, blocks_ref[1, frequency])
        sorted_ref[re_at : re_at + count] = (y[:count] - z[count:]).astype(jnp.bfloat16)
        sorted_ref[im_at : im_at + count] = (z[:count] + y[count:]).astype(jnp.bfloat16)

    product(1, 0, 2 * half, 2 * half)
    product(0, 4 * half, 6 * half, half)
    product(2, 5 * half, 7 * half, half)
    for third in range(thirds):
        at = third * groups
        rows = [sorted_ref[block * half + at : block * half + at + groups] for block in range(8)]
        put_rows(out_ref, third, mul(unsort_ref[...], jnp.concatenate(rows, axis=0)))


def carry_kernel(in_ref, residual_ref, jacobians_ref, pack_ref, unpack_ref,
                 following_ref, held_ref, send_ref):
    steps, columns, states = held_ref.shape
    thirds = in_ref.shape[1]
    width = columns // thirds
    for third in range(thirds):
        rows = mul(unpack_ref[...], rows_of(in_ref, third)).astype(jnp.bfloat16)
        following_ref[:, third * width : (third + 1) * width] = rows.reshape(steps, width, states)
    at_end = lax.axis_index("tm") == in_ref.shape[0] - 1
    for step in range(steps):
        carried = mul(following_ref[step], jacobians_ref[step])
        if step == steps - 1:
            carried = jnp.where(at_end, 0.0, 1.0) * carried
        held_ref[step] = residual_ref[step] + carried
    for third in range(thirds):
        rows = held_ref[:, third * width : (third + 1) * width].astype(jnp.bfloat16)
        put_rows(send_ref, third, mul(pack_ref[...], rows.reshape(steps * width, states)))


def finish_kernel(in_ref, following_ref, held_ref, jacobians_ref, unpack_ref, sort_ref,
                  adjoint_hbm, residual_hbm, adjoint_ref, residual_ref, sem):
    steps, columns, states = held_ref.shape
    thirds = in_ref.shape[1] - 1
    width = columns // thirds
    for third in range(thirds):
        rows = mul(unpack_ref[...], rows_of(in_ref, third))
        adjoint_ref[:, third * width : (third + 1) * width] = rows.reshape(steps, width, states)
    copies = []

    def put(index, source, target, step):
        copy = pltpu.make_async_copy(source.at[step], target.at[step], sem.at[index, step])
        copy.start()
        copies.append(copy)

    for step in range(steps):
        put(0, adjoint_ref, adjoint_hbm, step)
    for step in range(steps):
        if step + 1 < steps:
            following = adjoint_ref[step + 1] - following_ref[step].astype(jnp.float32)
            following = following.astype(jnp.bfloat16)
        else:
            following = mul(sort_ref[...], rows_of(in_ref, thirds))[:columns]
            following = following.astype(jnp.bfloat16)
        carried = mul(following, jacobians_ref[step])
        residual_ref[step] = held_ref[step] - (adjoint_ref[step] - carried)
        put(1, residual_ref, residual_hbm, step)
    for copy in copies:
        copy.wait()


def vmem():
    return pl.BlockSpec(memory_space=pltpu.VMEM)


def call(kernel, out_shape, args, limit, scratch=(), out_space=pltpu.VMEM, flops=1 << 28):
    return pl.pallas_call(
        kernel,
        out_shape=out_shape,
        in_specs=[vmem()] * len(args),
        out_specs=jax.tree.map(lambda _: pl.BlockSpec(memory_space=out_space), out_shape),
        scratch_shapes=list(scratch),
        compiler_params=pltpu.CompilerParams(vmem_limit_bytes=limit * MIB),
        cost_estimate=pl.CostEstimate(flops=flops, bytes_accessed=4 * MIB, transcendentals=0),
    )(*args)


def exchange(block):
    return lax.all_to_all(block, "tm", split_axis=0, concat_axis=0, tiled=True)


def body(objective, jacobians, precond_blocks):
    local_steps, columns, states = objective.shape
    groups = lax.axis_size("tm")
    steps = local_steps * groups
    thirds = columns // (2 * groups)
    width = columns // thirds
    forward, backward, forward_next, backward_next, beyond = tables(steps, groups)
    forward, backward, subtract_next, backward_next, beyond = (
        split_table(t) for t in (forward, backward, -forward_next, backward_next, beyond)
    )
    second = np.concatenate([forward, subtract_next], axis=1)
    both = np.concatenate([backward, backward], axis=1)
    pack, sort = shuffles(groups)
    unpack, unsort = pack.T.copy(), sort.T.copy()
    forward, second, both, backward_next, beyond, pack, unpack, sort, unsort = (
        jnp.asarray(t)
        for t in (forward, second, both, backward_next, beyond, pack, unpack, sort, unsort)
    )
    wire = jax.ShapeDtypeStruct((groups, thirds, 8, states), jnp.bfloat16)
    longer = jax.ShapeDtypeStruct((groups, thirds + 1, 8, states), jnp.bfloat16)
    field = jax.ShapeDtypeStruct(objective.shape, jnp.float32)
    plain = jax.ShapeDtypeStruct(objective.shape, jnp.bfloat16)

    def multiply(rows):
        return call(
            multiply_kernel,
            wire,
            (rows, sort, unsort, precond_blocks),
            PRODUCT_LIMIT,
            scratch=[pltpu.VMEM((4 * columns, states), jnp.bfloat16)],
            flops=1 << 31,
        )

    whole = lambda i: (0, 0)
    send, table = pl.pallas_call(
        pack_kernel,
        grid=(thirds,),
        out_shape=(wire, jax.ShapeDtypeStruct(forward.shape, forward.dtype)),
        in_specs=[
            pl.BlockSpec((local_steps, width, states), lambda i: (0, i, 0)),
            pl.BlockSpec(pack.shape, whole),
            pl.BlockSpec(forward.shape, whole),
        ],
        out_specs=(
            pl.BlockSpec((groups, 1, 8, states), lambda i: (0, i, 0, 0)),
            pl.BlockSpec(forward.shape, whole),
        ),
        compiler_params=pltpu.CompilerParams(vmem_limit_bytes=PACK_LIMIT * MIB),
    )(objective, pack, forward)
    rows = call(transform_kernel, wire, (exchange(send), table), 16)
    wave = exchange(multiply(exchange(rows)))
    ahead = call(transform_kernel, wire, (wave, backward_next), 16)
    following, held, send = call(
        carry_kernel,
        (plain, field, wire),
        (exchange(ahead), objective, jacobians, pack, unpack),
        16,
        flops=1 << 30,
    )
    rows = call(transform_kernel, wire, (exchange(send), ahead, second), 16)
    again = exchange(multiply(exchange(rows)))
    rows = call(last_transform_kernel, longer, (wave, again, both, beyond, unsort), 16)
    return call(
        finish_kernel,
        (field, field),
        (exchange(rows), following, held, jacobians, unpack, sort),
        16,
        scratch=[
            pltpu.VMEM(objective.shape, jnp.float32),
            pltpu.VMEM(objective.shape, jnp.float32),
            pltpu.SemaphoreType.DMA((2, local_steps)),
        ],
        out_space=pl.ANY,
        flops=1 << 30,
    )


def solution(mesh):
    in_specs = (P("tm", "obj", None), P("tm", None, None), P(None, "tm", None, None))
    out_specs = (P("tm", "obj", None), P("tm", "obj", None))
    return jax.shard_map(body, mesh=mesh, in_specs=in_specs, out_specs=out_specs, check_vma=False)
```

```python
import math

import jax
import jax.numpy as jnp
import numpy as np
from jax import lax
from jax.experimental import pallas as pl
from jax.experimental.pallas import tpu as pltpu
from jax.sharding import PartitionSpec as P

log_alpha = math.log(0.05)
MIB = 1 << 20


def split_table(table):
    high = table.astype(jnp.bfloat16)
    low = (table - high.astype(np.float64)).astype(jnp.bfloat16)
    return np.concatenate([high, low], axis=1)


def tables(steps, groups):
    local = steps // groups
    times = np.arange(steps)
    forward = np.zeros((groups, 2, 4, 2, steps))
    backward = np.zeros((2, steps, groups, 2, 4))
    grow = np.exp(times * (-log_alpha / steps))
    shrink = np.exp(times * (log_alpha / steps)) / steps
    for group in range(groups):
        low_side = group < groups // 2
        for position in range(2):
            first = (0 if low_side else 1) ^ position
            jobs = [(0, 4 * group + 1, position), (2, 4 * group + 2 * position, first)]
            for slot, frequency, half in jobs:
                angle = 2.0 * math.pi * ((frequency * times) % steps) / steps
                cosine, sine = np.cos(angle), np.sin(angle)
                if frequency % (steps // 2) == 0:
                    for at, part in ((slot, half), (slot + 1, 1 - half)):
                        forward[group, position, at, part] = cosine * grow
                        backward[part, :, group, position, at] = cosine * shrink
                    continue
                forward[group, position, slot, half] = cosine * grow
                forward[group, position, slot + 1, half] = -sine * grow
                backward[half, :, group, position, slot] = 2.0 * cosine * shrink
                backward[half, :, group, position, slot + 1] = -2.0 * sine * shrink
    size = 2 * steps
    forward = forward.reshape(size, 2, steps)
    backward = backward.reshape(2, steps, size)

    def by_owner(shift):
        ahead = np.roll(forward, -shift, axis=2).reshape(size, 2, groups, local)
        back = np.roll(backward, -shift, axis=1).reshape(2, groups, local, size)
        ahead = ahead.transpose(0, 2, 1, 3).reshape(size, size)
        return ahead, back.transpose(1, 0, 2, 3).reshape(size, size)

    beyond = np.concatenate([backward[:, local::local], np.zeros((2, 1, size))], axis=1)
    return (*by_owner(0), *by_owner(1), beyond.reshape(2 * groups, size))


def shuffles(groups):
    size = 8 * groups
    pack = np.zeros((groups, 2, 4, 4, 2, groups))
    sort = np.zeros((4, 2, groups, groups, 2, 4))
    for piece in range(groups):
        for half in range(2):
            for step in range(4):
                pack[piece, half, step, step, half, piece] = 1
                sort[step, half, piece, piece, half, step] = 1
    shape = (size, size)
    return pack.reshape(shape).astype(jnp.bfloat16), sort.reshape(shape).astype(jnp.bfloat16)


def mul(left, right):
    return jnp.dot(left, right, preferred_element_type=jnp.float32)


def rows_of(ref, third):
    groups, _, eight, states = ref.shape
    wide = ref[:, third].astype(jnp.float32)
    return wide.reshape(groups * eight, states).astype(jnp.bfloat16)


def put_rows(ref, third, rows):
    groups, _, eight, states = ref.shape
    ref[:, third] = rows.reshape(groups, eight, states).astype(ref.dtype)


def pack_kernel(objective_hbm, table_hbm, send_ref, table_ref, rows_ref, sem):
    groups, thirds, eight, states = send_ref.shape
    steps, columns, _ = rows_ref.shape
    width = columns // thirds
    copies = []
    for third in range(thirds):
        part = pl.ds(third * width, width)
        copies.append(
            pltpu.make_async_copy(objective_hbm.at[:, part], rows_ref.at[:, part], sem.at[third])
        )
        copies[-1].start()
    table_copy = pltpu.make_async_copy(table_hbm, table_ref, sem.at[thirds])
    table_copy.start()
    shape = (eight * groups, eight * groups)
    row = lax.broadcasted_iota(jnp.int32, shape, 0)
    source = (row % steps) * width + (row // steps % 2) * groups + row // eight
    pack = (source == lax.broadcasted_iota(jnp.int32, shape, 1)).astype(jnp.float32)
    pack = pack.astype(jnp.bfloat16)
    for third in range(thirds):
        copies[third].wait()
        rows = rows_ref[:, third * width : (third + 1) * width].astype(jnp.bfloat16)
        put_rows(send_ref, third, mul(pack, rows.reshape(steps * width, states)))
    table_copy.wait()


def transform_kernel(*refs):
    *in_refs, table_ref, out_ref = refs
    for third in range(out_ref.shape[1]):
        rows = []
        for in_ref in in_refs:
            rows += [rows_of(in_ref, third)] * 2
        put_rows(out_ref, third, mul(table_ref[...], jnp.concatenate(rows, axis=0)))


def last_transform_kernel(before_ref, in_ref, table_ref, beyond_ref, spread_ref, out_ref):
    groups, thirds = in_ref.shape[:2]
    extra = []
    for third in range(thirds):
        before, rows = rows_of(before_ref, third), rows_of(in_ref, third)
        rows = jnp.concatenate([before, before, rows, rows], axis=0)
        extra.append(mul(beyond_ref[...], rows).astype(jnp.bfloat16))
        put_rows(out_ref, third, mul(table_ref[...], rows))
    extra.append(jnp.zeros_like(extra[0]))
    put_rows(out_ref, thirds, mul(spread_ref[...], jnp.concatenate(extra, axis=0)))


def multiply_kernel(in_ref, sort_ref, unsort_ref, blocks_ref, out_ref, sorted_ref):
    groups, thirds, _, states = in_ref.shape
    half = thirds * groups
    for third in range(thirds):
        rows = mul(sort_ref[...], rows_of(in_ref, third)).astype(jnp.bfloat16)
        for block in range(8):
            at = block * half + third * groups
            sorted_ref[at : at + groups] = rows[block * groups : (block + 1) * groups]

    def product(frequency, re_at, im_at, count):
        left = jnp.concatenate(
            [sorted_ref[re_at : re_at + count], sorted_ref[im_at : im_at + count]], axis=0
        )
        y = mul(left, blocks_ref[0, frequency])
        z = mul(left, blocks_ref[1, frequency])
        sorted_ref[re_at : re_at + count] = (y[:count] - z[count:]).astype(jnp.bfloat16)
        sorted_ref[im_at : im_at + count] = (z[:count] + y[count:]).astype(jnp.bfloat16)

    product(1, 0, 2 * half, 2 * half)
    product(0, 4 * half, 6 * half, half)
    product(2, 5 * half, 7 * half, half)
    for third in range(thirds):
        at = third * groups
        rows = [sorted_ref[block * half + at : block * half + at + groups] for block in range(8)]
        put_rows(out_ref, third, mul(unsort_ref[...], jnp.concatenate(rows, axis=0)))


def carry_kernel(in_ref, objective_ref, jacobians_ref, pack_ref, unpack_ref, send_ref,
                 following_ref, sum_ref):
    steps, columns, states = objective_ref.shape
    thirds = in_ref.shape[1]
    width = columns // thirds
    for third in range(thirds):
        rows = mul(unpack_ref[...], rows_of(in_ref, third)).astype(jnp.bfloat16)
        following_ref[:, third * width : (third + 1) * width] = rows.reshape(steps, width, states)
    at_end = lax.axis_index("tm") == in_ref.shape[0] - 1
    for step in range(steps):
        carried = mul(following_ref[step], jacobians_ref[step])
        if step == steps - 1:
            carried = jnp.where(at_end, 0.0, 1.0) * carried
        sum_ref[step] = (objective_ref[step] + carried).astype(jnp.bfloat16)
    for third in range(thirds):
        rows = sum_ref[:, third * width : (third + 1) * width]
        put_rows(send_ref, third, mul(pack_ref[...], rows.reshape(steps * width, states)))


def finish_kernel(in_ref, objective_ref, jacobians_ref, unpack_ref, sort_ref,
                  adjoint_hbm, residual_hbm, adjoint_ref, residual_ref, sem):
    steps, columns, states = objective_ref.shape
    thirds = in_ref.shape[1] - 1
    width = columns // thirds
    copies = []

    def put(source, target, part, flag):
        copies.append(pltpu.make_async_copy(source.at[part], target.at[part], flag))
        copies[-1].start()

    for third in range(thirds):
        rows = mul(unpack_ref[...], rows_of(in_ref, third))
        adjoint_ref[:, third * width : (third + 1) * width] = rows.reshape(steps, width, states)
        part = (slice(None), pl.ds(third * width, width))
        put(adjoint_ref, adjoint_hbm, part, sem.at[0, third])
    for step in range(steps):
        if step + 1 < steps:
            following = adjoint_ref[step + 1].astype(jnp.bfloat16)
        else:
            following = mul(sort_ref[...], rows_of(in_ref, thirds))[:columns]
            following = following.astype(jnp.bfloat16)
        carried = mul(following, jacobians_ref[step])
        residual_ref[step] = objective_ref[step] - (adjoint_ref[step] - carried)
        put(residual_ref, residual_hbm, step, sem.at[1, step])
    for copy in copies:
        copy.wait()


def call(kernel, out_shape, args, limit, scratch=(), in_space=pltpu.VMEM,
         out_space=pltpu.VMEM, flops=1 << 28):
    return pl.pallas_call(
        kernel,
        out_shape=out_shape,
        in_specs=[pl.BlockSpec(memory_space=in_space)] * len(args),
        out_specs=jax.tree.map(lambda _: pl.BlockSpec(memory_space=out_space), out_shape),
        scratch_shapes=list(scratch),
        compiler_params=pltpu.CompilerParams(vmem_limit_bytes=limit * MIB),
        cost_estimate=pl.CostEstimate(flops=flops, bytes_accessed=4 * MIB, transcendentals=0),
    )(*args)


def exchange(block):
    return lax.all_to_all(block, "tm", split_axis=0, concat_axis=0, tiled=True)


def body(objective, jacobians, precond_blocks):
    local_steps, columns, states = objective.shape
    groups = lax.axis_size("tm")
    steps = local_steps * groups
    thirds = columns // (2 * groups)
    forward, backward, forward_next, backward_next, beyond = tables(steps, groups)
    forward, backward, subtract_next, backward_next, beyond = (
        split_table(t) for t in (forward, backward, -forward_next, backward_next, beyond)
    )
    second = np.concatenate([forward, subtract_next], axis=1)
    both = np.concatenate([backward, backward], axis=1)
    beyond = np.concatenate([beyond, beyond], axis=1)
    pack, sort = shuffles(groups)
    unpack, unsort = pack.T.copy(), sort.T.copy()
    forward, second, both, backward_next, beyond, pack, unpack, sort, unsort = (
        jnp.asarray(t)
        for t in (forward, second, both, backward_next, beyond, pack, unpack, sort, unsort)
    )
    wire = jax.ShapeDtypeStruct((groups, thirds, 8, states), jnp.bfloat16)
    longer = jax.ShapeDtypeStruct((groups, thirds + 1, 8, states), jnp.bfloat16)
    field = jax.ShapeDtypeStruct(objective.shape, jnp.float32)

    def multiply(rows):
        return call(
            multiply_kernel,
            wire,
            (rows, sort, unsort, precond_blocks),
            16,
            scratch=[pltpu.VMEM((4 * columns, states), jnp.bfloat16)],
            flops=1 << 31,
        )

    send, table = call(
        pack_kernel,
        (wire, jax.ShapeDtypeStruct(forward.shape, forward.dtype)),
        (objective, forward),
        16,
        scratch=[
            pltpu.VMEM(objective.shape, jnp.float32),
            pltpu.SemaphoreType.DMA((thirds + 1,)),
        ],
        in_space=pltpu.HBM,
    )
    rows = call(transform_kernel, wire, (exchange(send), table), 16)
    wave = exchange(multiply(exchange(rows)))
    ahead = call(transform_kernel, wire, (wave, backward_next), 16)
    send = call(
        carry_kernel,
        wire,
        (exchange(ahead), objective, jacobians, pack, unpack),
        16,
        scratch=[pltpu.VMEM(objective.shape, jnp.bfloat16)] * 2,
        flops=1 << 30,
    )
    rows = call(transform_kernel, wire, (exchange(send), ahead, second), 16)
    again = exchange(multiply(exchange(rows)))
    rows = call(last_transform_kernel, longer, (wave, again, both, beyond, unsort), 16)
    return call(
        finish_kernel,
        (field, field),
        (exchange(rows), objective, jacobians, unpack, sort),
        16,
        scratch=[
            pltpu.VMEM(objective.shape, jnp.float32),
            pltpu.VMEM(objective.shape, jnp.float32),
            pltpu.SemaphoreType.DMA((2, local_steps)),
        ],
        out_space=pl.ANY,
        flops=1 << 30,
    )


def solution(mesh):
    in_specs = (P("tm", "obj", None), P("tm", None, None), P(None, "tm", None, None))
    out_specs = (P("tm", "obj", None), P("tm", "obj", None))
    return jax.shard_map(body, mesh=mesh, in_specs=in_specs, out_specs=out_specs, check_vma=False)
```

```python
import math

import jax
import jax.numpy as jnp
import numpy as np
from jax import lax
from jax.experimental import pallas as pl
from jax.experimental.pallas import tpu as pltpu
from jax.sharding import PartitionSpec as P

log_alpha = math.log(0.05)
MIB = 1 << 20


def split_table(table):
    high = table.astype(jnp.bfloat16)
    low = (table - high.astype(np.float64)).astype(jnp.bfloat16)
    return np.concatenate([high, low], axis=1)


def tables(steps, groups):
    local = steps // groups
    times = np.arange(steps)
    forward = np.zeros((groups, 2, 4, 2, steps))
    backward = np.zeros((2, steps, groups, 2, 4))
    grow = np.exp(times * (-log_alpha / steps))
    shrink = np.exp(times * (log_alpha / steps)) / steps
    for group in range(groups):
        low_side = group < groups // 2
        for position in range(2):
            first = (0 if low_side else 1) ^ position
            jobs = [(0, 4 * group + 1, position), (2, 4 * group + 2 * position, first)]
            for slot, frequency, half in jobs:
                angle = 2.0 * math.pi * ((frequency * times) % steps) / steps
                cosine, sine = np.cos(angle), np.sin(angle)
                if frequency % (steps // 2) == 0:
                    for at, part in ((slot, half), (slot + 1, 1 - half)):
                        forward[group, position, at, part] = cosine * grow
                        backward[part, :, group, position, at] = cosine * shrink
                    continue
                forward[group, position, slot, half] = cosine * grow
                forward[group, position, slot + 1, half] = -sine * grow
                backward[half, :, group, position, slot] = 2.0 * cosine * shrink
                backward[half, :, group, position, slot + 1] = -2.0 * sine * shrink
    size = 2 * steps
    forward = forward.reshape(size, 2, steps)
    backward = backward.reshape(2, steps, size)

    def by_owner(shift):
        ahead = np.roll(forward, -shift, axis=2).reshape(size, 2, groups, local)
        back = np.roll(backward, -shift, axis=1).reshape(2, groups, local, size)
        ahead = ahead.transpose(0, 2, 1, 3).reshape(size, size)
        return ahead, back.transpose(1, 0, 2, 3).reshape(size, size)

    beyond = np.concatenate([backward[:, local::local], np.zeros((2, 1, size))], axis=1)
    return (*by_owner(0), *by_owner(1), beyond.reshape(2 * groups, size))


def shuffles(groups):
    size = 8 * groups
    pack = np.zeros((groups, 2, 4, 4, 2, groups))
    sort = np.zeros((4, 2, groups, groups, 2, 4))
    for piece in range(groups):
        for half in range(2):
            for step in range(4):
                pack[piece, half, step, step, half, piece] = 1
                sort[step, half, piece, piece, half, step] = 1
    shape = (size, size)
    return pack.reshape(shape).astype(jnp.bfloat16), sort.reshape(shape).astype(jnp.bfloat16)


def mul(left, right):
    return jnp.dot(left, right, preferred_element_type=jnp.float32)


def rows_of(ref, third):
    groups, _, eight, states = ref.shape
    return ref[:, third].reshape(groups * eight, states)


def put_rows(ref, third, rows):
    groups, _, eight, states = ref.shape
    ref[:, third] = rows.reshape(groups, eight, states).astype(ref.dtype)


def pack_kernel(objective_ref, send_ref):
    groups, thirds, eight, states = send_ref.shape
    steps, columns, _ = objective_ref.shape
    width = columns // thirds
    shape = (eight * groups, eight * groups)
    row = lax.broadcasted_iota(jnp.int32, shape, 0)
    source = (row % steps) * width + (row // steps % 2) * groups + row // eight
    pack = (source == lax.broadcasted_iota(jnp.int32, shape, 1)).astype(jnp.float32)
    pack = pack.astype(jnp.bfloat16)
    for third in range(thirds):
        rows = objective_ref[:, third * width : (third + 1) * width].astype(jnp.bfloat16)
        put_rows(send_ref, third, mul(pack, rows.reshape(steps * width, states)))


def transform_kernel(*refs):
    *in_refs, table_ref, out_ref = refs
    for third in range(out_ref.shape[1]):
        rows = []
        for in_ref in in_refs:
            rows += [rows_of(in_ref, third)] * 2
        put_rows(out_ref, third, mul(table_ref[...], jnp.concatenate(rows, axis=0)))


def last_transform_kernel(before_ref, in_ref, table_ref, spread_ref, out_ref):
    groups, thirds, eight, _ = in_ref.shape
    extra = []
    for third in range(thirds):
        before, rows = rows_of(before_ref, third), rows_of(in_ref, third)
        rows = jnp.concatenate([before, before, rows, rows], axis=0)
        rows = mul(table_ref[...], rows)
        extra.append(rows[eight * groups :].astype(jnp.bfloat16))
        put_rows(out_ref, third, rows[: eight * groups])
    extra.append(jnp.zeros_like(extra[0]))
    put_rows(out_ref, thirds, mul(spread_ref[...], jnp.concatenate(extra, axis=0)))


def multiply_kernel(in_ref, sort_ref, unsort_ref, blocks_ref, out_ref, sorted_ref):
    groups, thirds, _, states = in_ref.shape
    half = thirds * groups
    for third in range(thirds):
        rows = mul(sort_ref[...], rows_of(in_ref, third)).astype(jnp.bfloat16)
        for block in range(8):
            at = block * half + third * groups
            sorted_ref[at : at + groups] = rows[block * groups : (block + 1) * groups]

    def product(frequency, re_at, im_at, count):
        left = jnp.concatenate(
            [sorted_ref[re_at : re_at + count], sorted_ref[im_at : im_at + count]], axis=0
        )
        y = mul(left, blocks_ref[0, frequency])
        z = mul(left, blocks_ref[1, frequency])
        sorted_ref[re_at : re_at + count] = (y[:count] - z[count:]).astype(jnp.bfloat16)
        sorted_ref[im_at : im_at + count] = (z[:count] + y[count:]).astype(jnp.bfloat16)

    product(1, 0, 2 * half, 2 * half)
    product(0, 4 * half, 6 * half, half)
    product(2, 5 * half, 7 * half, half)
    for third in range(thirds):
        at = third * groups
        rows = [sorted_ref[block * half + at : block * half + at + groups] for block in range(8)]
        put_rows(out_ref, third, mul(unsort_ref[...], jnp.concatenate(rows, axis=0)))


def carry_kernel(in_ref, objective_ref, jacobians_ref, pack_ref, unpack_ref, send_ref,
                 following_ref, sum_ref):
    steps, columns, states = objective_ref.shape
    thirds = in_ref.shape[1]
    width = columns // thirds
    for third in range(thirds):
        rows = mul(unpack_ref[...], rows_of(in_ref, third)).astype(jnp.bfloat16)
        following_ref[:, third * width : (third + 1) * width] = rows.reshape(steps, width, states)
    at_end = lax.axis_index("tm") == in_ref.shape[0] - 1
    for step in range(steps):
        carried = mul(following_ref[step], jacobians_ref[step])
        if step == steps - 1:
            carried = jnp.where(at_end, 0.0, 1.0) * carried
        sum_ref[step] = (objective_ref[step] + carried).astype(jnp.bfloat16)
    for third in range(thirds):
        rows = sum_ref[:, third * width : (third + 1) * width]
        put_rows(send_ref, third, mul(pack_ref[...], rows.reshape(steps * width, states)))


def finish_kernel(in_ref, objective_ref, jacobians_ref, unpack_ref, sort_ref,
                  adjoint_hbm, residual_hbm, adjoint_ref, residual_ref, sem):
    steps, columns, states = objective_ref.shape
    thirds = in_ref.shape[1] - 1
    width = columns // thirds
    copies = []

    def put(source, target, part, flag):
        copies.append(pltpu.make_async_copy(source.at[part], target.at[part], flag))
        copies[-1].start()

    for third in range(thirds):
        rows = mul(unpack_ref[...], rows_of(in_ref, third))
        adjoint_ref[:, third * width : (third + 1) * width] = rows.reshape(steps, width, states)
        part = (slice(None), pl.ds(third * width, width))
        put(adjoint_ref, adjoint_hbm, part, sem.at[0, third])
    for step in range(steps):
        if step + 1 < steps:
            following = adjoint_ref[step + 1].astype(jnp.bfloat16)
        else:
            following = mul(sort_ref[...], rows_of(in_ref, thirds))[:columns]
            following = following.astype(jnp.bfloat16)
        carried = mul(following, jacobians_ref[step])
        residual_ref[step] = objective_ref[step] - (adjoint_ref[step] - carried)
        put(residual_ref, residual_hbm, step, sem.at[1, step])
    for copy in copies:
        copy.wait()


def call(kernel, out_shape, args, limit, scratch=(), out_space=pltpu.VMEM, flops=1 << 28):
    return pl.pallas_call(
        kernel,
        out_shape=out_shape,
        in_specs=[pl.BlockSpec(memory_space=pltpu.VMEM)] * len(args),
        out_specs=jax.tree.map(lambda _: pl.BlockSpec(memory_space=out_space), out_shape),
        scratch_shapes=list(scratch),
        compiler_params=pltpu.CompilerParams(vmem_limit_bytes=limit * MIB),
        cost_estimate=pl.CostEstimate(flops=flops, bytes_accessed=4 * MIB, transcendentals=0),
    )(*args)


def exchange(block):
    return lax.all_to_all(block, "tm", split_axis=0, concat_axis=0, tiled=True)


def body(objective, jacobians, precond_blocks):
    local_steps, columns, states = objective.shape
    groups = lax.axis_size("tm")
    steps = local_steps * groups
    thirds = columns // (2 * groups)
    forward, backward, forward_next, backward_next, beyond = tables(steps, groups)
    forward, backward, subtract_next, backward_next, beyond = (
        split_table(t) for t in (forward, backward, -forward_next, backward_next, beyond)
    )
    second = np.concatenate([forward, subtract_next], axis=1)
    both = np.concatenate([backward, beyond], axis=0)
    both = np.concatenate([both, both], axis=1)
    pack, sort = shuffles(groups)
    unpack, unsort = pack.T.copy(), sort.T.copy()
    forward, second, both, backward_next, pack, unpack, sort, unsort = (
        jnp.asarray(t)
        for t in (forward, second, both, backward_next, pack, unpack, sort, unsort)
    )
    wire = jax.ShapeDtypeStruct((groups, thirds, 8, states), jnp.bfloat16)
    longer = jax.ShapeDtypeStruct((groups, thirds + 1, 8, states), jnp.bfloat16)
    field = jax.ShapeDtypeStruct(objective.shape, jnp.float32)

    def multiply(rows):
        return call(
            multiply_kernel,
            wire,
            (rows, sort, unsort, precond_blocks),
            16,
            scratch=[pltpu.VMEM((4 * columns, states), jnp.bfloat16)],
            flops=1 << 31,
        )

    send = call(pack_kernel, wire, (objective,), 16)
    rows = call(transform_kernel, wire, (exchange(send), forward), 16)
    wave = exchange(multiply(exchange(rows)))
    ahead = call(transform_kernel, wire, (wave, backward_next), 16)
    send = call(
        carry_kernel,
        wire,
        (exchange(ahead), objective, jacobians, pack, unpack),
        16,
        scratch=[pltpu.VMEM(objective.shape, jnp.bfloat16)] * 2,
        flops=1 << 30,
    )
    rows = call(transform_kernel, wire, (exchange(send), ahead, second), 16)
    again = exchange(multiply(exchange(rows)))
    rows = call(last_transform_kernel, longer, (wave, again, both, unsort), 16)
    return call(
        finish_kernel,
        (field, field),
        (exchange(rows), objective, jacobians, unpack, sort),
        16,
        scratch=[
            pltpu.VMEM(objective.shape, jnp.float32),
            pltpu.VMEM(objective.shape, jnp.float32),
            pltpu.SemaphoreType.DMA((2, local_steps)),
        ],
        out_space=pl.ANY,
        flops=1 << 30,
    )


def solution(mesh):
    in_specs = (P("tm", "obj", None), P("tm", None, None), P(None, "tm", None, None))
    out_specs = (P("tm", "obj", None), P("tm", "obj", None))
    return jax.shard_map(body, mesh=mesh, in_specs=in_specs, out_specs=out_specs, check_vma=False)
```

```python
import math

import jax
import jax.numpy as jnp
import numpy as np
from jax import lax
from jax.experimental import pallas as pl
from jax.experimental.pallas import tpu as pltpu
from jax.sharding import PartitionSpec as P

log_alpha = math.log(0.05)
MIB = 1 << 20


def split_table(table):
    high = table.astype(jnp.bfloat16)
    low = (table - high.astype(np.float64)).astype(jnp.bfloat16)
    return np.concatenate([high, low], axis=1)


def tables(steps, groups):
    local = steps // groups
    times = np.arange(steps)
    forward = np.zeros((groups, 2, 4, 2, steps))
    backward = np.zeros((2, steps, groups, 2, 4))
    grow = np.exp(times * (-log_alpha / steps))
    shrink = np.exp(times * (log_alpha / steps)) / steps
    for group in range(groups):
        low_side = group < groups // 2
        for position in range(2):
            first = (0 if low_side else 1) ^ position
            jobs = [(0, 4 * group + 1, position), (2, 4 * group + 2 * position, first)]
            for slot, frequency, half in jobs:
                angle = 2.0 * math.pi * ((frequency * times) % steps) / steps
                cosine, sine = np.cos(angle), np.sin(angle)
                if frequency % (steps // 2) == 0:
                    for at, part in ((slot, half), (slot + 1, 1 - half)):
                        forward[group, position, at, part] = cosine * grow
                        backward[part, :, group, position, at] = cosine * shrink
                    continue
                forward[group, position, slot, half] = cosine * grow
                forward[group, position, slot + 1, half] = -sine * grow
                backward[half, :, group, position, slot] = 2.0 * cosine * shrink
                backward[half, :, group, position, slot + 1] = -2.0 * sine * shrink
    size = 2 * steps
    forward = forward.reshape(size, 2, steps)
    backward = backward.reshape(2, steps, size)

    def by_owner(shift):
        ahead = np.roll(forward, -shift, axis=2).reshape(size, 2, groups, local)
        back = np.roll(backward, -shift, axis=1).reshape(2, groups, local, size)
        ahead = ahead.transpose(0, 2, 1, 3).reshape(size, size)
        return ahead, back.transpose(1, 0, 2, 3).reshape(size, size)

    beyond = np.concatenate([backward[:, local::local], np.zeros((2, 1, size))], axis=1)
    return (*by_owner(0), *by_owner(1), beyond.reshape(2 * groups, size))


def shuffles(groups):
    size = 8 * groups
    pack = np.zeros((groups, 2, 4, 4, 2, groups))
    sort = np.zeros((4, 2, groups, groups, 2, 4))
    for piece in range(groups):
        for half in range(2):
            for step in range(4):
                pack[piece, half, step, step, half, piece] = 1
                sort[step, half, piece, piece, half, step] = 1
    shape = (size, size)
    return pack.reshape(shape).astype(jnp.bfloat16), sort.reshape(shape).astype(jnp.bfloat16)


def mul(left, right):
    return jnp.dot(left, right, preferred_element_type=jnp.float32)


def rows_of(ref, third):
    groups, _, eight, states = ref.shape
    return ref[:, third].reshape(groups * eight, states)


def put_rows(ref, third, rows):
    groups, _, eight, states = ref.shape
    ref[:, third] = rows.reshape(groups, eight, states).astype(ref.dtype)


def pack_kernel(objective_ref, send_ref):
    groups, thirds, eight, states = send_ref.shape
    steps, columns, _ = objective_ref.shape
    width = columns // thirds
    shape = (eight * groups, eight * groups)
    row = lax.broadcasted_iota(jnp.int32, shape, 0)
    source = (row % steps) * width + (row // steps % 2) * groups + row // eight
    pack = (source == lax.broadcasted_iota(jnp.int32, shape, 1)).astype(jnp.float32)
    pack = pack.astype(jnp.bfloat16)
    for third in range(thirds):
        rows = objective_ref[:, third * width : (third + 1) * width].astype(jnp.bfloat16)
        put_rows(send_ref, third, mul(pack, rows.reshape(steps * width, states)))


def transform_kernel(*refs):
    *in_refs, table_ref, out_ref = refs
    for third in range(out_ref.shape[1]):
        rows = []
        for in_ref in in_refs:
            rows += [rows_of(in_ref, third)] * 2
        put_rows(out_ref, third, mul(table_ref[...], jnp.concatenate(rows, axis=0)))


def last_transform_kernel(before_ref, in_ref, table_ref, spread_ref, out_ref):
    groups, thirds, eight, _ = in_ref.shape
    extra = []
    for third in range(thirds):
        before, rows = rows_of(before_ref, third), rows_of(in_ref, third)
        rows = jnp.concatenate([before, before, rows, rows], axis=0)
        rows = mul(table_ref[...], rows)
        extra.append(rows[eight * groups :].astype(jnp.bfloat16))
        put_rows(out_ref, third, rows[: eight * groups])
    extra.append(jnp.zeros_like(extra[0]))
    put_rows(out_ref, thirds, mul(spread_ref[...], jnp.concatenate(extra, axis=0)))


def multiply_kernel(in_ref, sort_ref, unsort_ref, blocks_ref, out_ref, sorted_ref):
    groups, thirds, _, states = in_ref.shape
    half = thirds * groups
    for third in range(thirds):
        rows = mul(sort_ref[...], rows_of(in_ref, third)).astype(jnp.bfloat16)
        for block in range(8):
            at = block * half + third * groups
            sorted_ref[at : at + groups] = rows[block * groups : (block + 1) * groups]

    def product(frequency, re_at, im_at, count):
        re = sorted_ref[re_at : re_at + count]
        im = sorted_ref[im_at : im_at + count]
        left = jnp.concatenate(
            [jnp.concatenate([re, -im], axis=1), jnp.concatenate([im, re], axis=1)], axis=0
        )
        right = jnp.concatenate([blocks_ref[0, frequency], blocks_ref[1, frequency]], axis=0)
        rows = mul(left, right).astype(jnp.bfloat16)
        sorted_ref[re_at : re_at + count] = rows[:count]
        sorted_ref[im_at : im_at + count] = rows[count:]

    product(1, 0, 2 * half, 2 * half)
    product(0, 4 * half, 6 * half, half)
    product(2, 5 * half, 7 * half, half)
    for third in range(thirds):
        at = third * groups
        rows = [sorted_ref[block * half + at : block * half + at + groups] for block in range(8)]
        put_rows(out_ref, third, mul(unsort_ref[...], jnp.concatenate(rows, axis=0)))


def carry_kernel(in_ref, objective_ref, jacobians_ref, pack_ref, unpack_ref, send_ref,
                 following_ref, sum_ref):
    steps, columns, states = objective_ref.shape
    thirds = in_ref.shape[1]
    width = columns // thirds
    for third in range(thirds):
        rows = mul(unpack_ref[...], rows_of(in_ref, third)).astype(jnp.bfloat16)
        following_ref[:, third * width : (third + 1) * width] = rows.reshape(steps, width, states)
    at_end = lax.axis_index("tm") == in_ref.shape[0] - 1
    for step in range(steps):
        carried = mul(following_ref[step], jacobians_ref[step])
        if step == steps - 1:
            carried = jnp.where(at_end, 0.0, 1.0) * carried
        sum_ref[step] = (objective_ref[step] + carried).astype(jnp.bfloat16)
    for third in range(thirds):
        rows = sum_ref[:, third * width : (third + 1) * width]
        put_rows(send_ref, third, mul(pack_ref[...], rows.reshape(steps * width, states)))


def finish_kernel(in_ref, objective_ref, jacobians_ref, unpack_ref, sort_ref,
                  adjoint_hbm, residual_hbm, adjoint_ref, residual_ref, sem):
    steps, columns, states = objective_ref.shape
    thirds = in_ref.shape[1] - 1
    width = columns // thirds
    copies = []

    def put(source, target, part, flag):
        copies.append(pltpu.make_async_copy(source.at[part], target.at[part], flag))
        copies[-1].start()

    for third in range(thirds):
        rows = mul(unpack_ref[...], rows_of(in_ref, third))
        adjoint_ref[:, third * width : (third + 1) * width] = rows.reshape(steps, width, states)
        part = (slice(None), pl.ds(third * width, width))
        put(adjoint_ref, adjoint_hbm, part, sem.at[0, third])
    for step in range(steps):
        if step + 1 < steps:
            following = adjoint_ref[step + 1].astype(jnp.bfloat16)
        else:
            following = mul(sort_ref[...], rows_of(in_ref, thirds))[:columns]
            following = following.astype(jnp.bfloat16)
        carried = mul(following, jacobians_ref[step])
        residual_ref[step] = objective_ref[step] - (adjoint_ref[step] - carried)
        put(residual_ref, residual_hbm, step, sem.at[1, step])
    for copy in copies:
        copy.wait()


def call(kernel, out_shape, args, limit, scratch=(), out_space=pltpu.VMEM, flops=1 << 28):
    return pl.pallas_call(
        kernel,
        out_shape=out_shape,
        in_specs=[pl.BlockSpec(memory_space=pltpu.VMEM)] * len(args),
        out_specs=jax.tree.map(lambda _: pl.BlockSpec(memory_space=out_space), out_shape),
        scratch_shapes=list(scratch),
        compiler_params=pltpu.CompilerParams(vmem_limit_bytes=limit * MIB),
        cost_estimate=pl.CostEstimate(flops=flops, bytes_accessed=4 * MIB, transcendentals=0),
    )(*args)


def exchange(block):
    return lax.all_to_all(block, "tm", split_axis=0, concat_axis=0, tiled=True)


def body(objective, jacobians, precond_blocks):
    local_steps, columns, states = objective.shape
    groups = lax.axis_size("tm")
    steps = local_steps * groups
    thirds = columns // (2 * groups)
    forward, backward, forward_next, backward_next, beyond = tables(steps, groups)
    forward, backward, subtract_next, backward_next, beyond = (
        split_table(t) for t in (forward, backward, -forward_next, backward_next, beyond)
    )
    second = np.concatenate([forward, subtract_next], axis=1)
    both = np.concatenate([backward, beyond], axis=0)
    both = np.concatenate([both, both], axis=1)
    pack, sort = shuffles(groups)
    unpack, unsort = pack.T.copy(), sort.T.copy()
    forward, second, both, backward_next, pack, unpack, sort, unsort = (
        jnp.asarray(t)
        for t in (forward, second, both, backward_next, pack, unpack, sort, unsort)
    )
    wire = jax.ShapeDtypeStruct((groups, thirds, 8, states), jnp.bfloat16)
    longer = jax.ShapeDtypeStruct((groups, thirds + 1, 8, states), jnp.bfloat16)
    field = jax.ShapeDtypeStruct(objective.shape, jnp.float32)

    def multiply(rows):
        return call(
            multiply_kernel,
            wire,
            (rows, sort, unsort, precond_blocks),
            16,
            scratch=[pltpu.VMEM((4 * columns, states), jnp.bfloat16)],
            flops=1 << 31,
        )

    send = call(pack_kernel, wire, (objective,), 16)
    rows = call(transform_kernel, wire, (exchange(send), forward), 16)
    wave = exchange(multiply(exchange(rows)))
    ahead = call(transform_kernel, wire, (wave, backward_next), 16)
    send = call(
        carry_kernel,
        wire,
        (exchange(ahead), objective, jacobians, pack, unpack),
        16,
        scratch=[pltpu.VMEM(objective.shape, jnp.bfloat16)] * 2,
        flops=1 << 30,
    )
    rows = call(transform_kernel, wire, (exchange(send), ahead, second), 16)
    again = exchange(multiply(exchange(rows)))
    rows = call(last_transform_kernel, longer, (wave, again, both, unsort), 16)
    return call(
        finish_kernel,
        (field, field),
        (exchange(rows), objective, jacobians, unpack, sort),
        16,
        scratch=[
            pltpu.VMEM(objective.shape, jnp.float32),
            pltpu.VMEM(objective.shape, jnp.float32),
            pltpu.SemaphoreType.DMA((2, local_steps)),
        ],
        out_space=pl.ANY,
        flops=1 << 30,
    )


def solution(mesh):
    in_specs = (P("tm", "obj", None), P("tm", None, None), P(None, "tm", None, None))
    out_specs = (P("tm", "obj", None), P("tm", "obj", None))
    return jax.shard_map(body, mesh=mesh, in_specs=in_specs, out_specs=out_specs, check_vma=False)
```

```python
import math

import jax
import jax.numpy as jnp
import numpy as np
from jax import lax
from jax.experimental import pallas as pl
from jax.experimental.pallas import tpu as pltpu
from jax.sharding import PartitionSpec as P

log_alpha = math.log(0.05)
MIB = 1 << 20


def split_table(table):
    high = table.astype(jnp.bfloat16)
    low = (table - high.astype(np.float64)).astype(jnp.bfloat16)
    return np.concatenate([high, low], axis=0)


def tables(steps, groups):
    local = steps // groups
    times = np.arange(steps)
    forward = np.zeros((groups, 2, 4, 2, steps))
    backward = np.zeros((2, steps, groups, 2, 4))
    grow = np.exp(times * (-log_alpha / steps))
    shrink = np.exp(times * (log_alpha / steps)) / steps
    for group in range(groups):
        low_side = group < groups // 2
        for position in range(2):
            first = (0 if low_side else 1) ^ position
            jobs = [(0, 4 * group + 1, position), (2, 4 * group + 2 * position, first)]
            for slot, frequency, half in jobs:
                angle = 2.0 * math.pi * ((frequency * times) % steps) / steps
                cosine, sine = np.cos(angle), np.sin(angle)
                if frequency % (steps // 2) == 0:
                    for at, part in ((slot, half), (slot + 1, 1 - half)):
                        forward[group, position, at, part] = cosine * grow
                        backward[part, :, group, position, at] = cosine * shrink
                    continue
                forward[group, position, slot, half] = cosine * grow
                forward[group, position, slot + 1, half] = -sine * grow
                backward[half, :, group, position, slot] = 2.0 * cosine * shrink
                backward[half, :, group, position, slot + 1] = -2.0 * sine * shrink
    size = 2 * steps
    forward = forward.reshape(size, 2, steps)
    backward = backward.reshape(2, steps, size)

    def by_owner(shift):
        ahead = np.roll(forward, -shift, axis=2).reshape(size, 2, groups, local)
        back = np.roll(backward, -shift, axis=1).reshape(2, groups, local, size)
        ahead = ahead.transpose(0, 2, 1, 3).reshape(size, size)
        return ahead, back.transpose(1, 0, 2, 3).reshape(size, size)

    beyond = np.concatenate([backward[:, local::local], np.zeros((2, 1, size))], axis=1)
    return (*by_owner(0), *by_owner(1), beyond.reshape(2 * groups, size))


def shuffles(groups):
    size = 8 * groups
    pack = np.zeros((groups, 2, 4, 4, 2, groups))
    sort = np.zeros((4, 2, groups, groups, 2, 4))
    for piece in range(groups):
        for half in range(2):
            for step in range(4):
                pack[piece, half, step, step, half, piece] = 1
                sort[step, half, piece, piece, half, step] = 1
    shape = (size, size)
    return pack.reshape(shape).astype(jnp.bfloat16), sort.reshape(shape).astype(jnp.bfloat16)


def mul(left, right):
    return jnp.dot(left, right, preferred_element_type=jnp.float32)


def rows_of(ref, third):
    groups, _, eight, states = ref.shape
    return ref[:, third].reshape(groups * eight, states)


def put_rows(ref, third, rows):
    groups, _, eight, states = ref.shape
    ref[:, third] = rows.reshape(groups, eight, states).astype(ref.dtype)


def pack_kernel(objective_ref, send_ref):
    groups, thirds, eight, states = send_ref.shape
    steps, columns, _ = objective_ref.shape
    width = columns // thirds
    shape = (eight * groups, eight * groups)
    row = lax.broadcasted_iota(jnp.int32, shape, 0)
    source = (row % steps) * width + (row // steps % 2) * groups + row // eight
    pack = (source == lax.broadcasted_iota(jnp.int32, shape, 1)).astype(jnp.float32)
    pack = pack.astype(jnp.bfloat16)
    for third in range(thirds):
        rows = objective_ref[:, third * width : (third + 1) * width].astype(jnp.bfloat16)
        put_rows(send_ref, third, mul(pack, rows.reshape(steps * width, states)))


def apply_table(table_ref, rows):
    both = mul(table_ref[...], rows)
    count = both.shape[0] // 2
    return both[:count] + both[count:]


def transform_kernel(*refs):
    *in_refs, table_ref, out_ref = refs
    for third in range(out_ref.shape[1]):
        rows = [rows_of(in_ref, third) for in_ref in in_refs]
        put_rows(out_ref, third, apply_table(table_ref, jnp.concatenate(rows, axis=0)))


def last_transform_kernel(before_ref, in_ref, table_ref, spread_ref, out_ref):
    groups, thirds, eight, _ = in_ref.shape
    extra = []
    for third in range(thirds):
        rows = [rows_of(before_ref, third), rows_of(in_ref, third)]
        rows = apply_table(table_ref, jnp.concatenate(rows, axis=0))
        extra.append(rows[eight * groups :].astype(jnp.bfloat16))
        put_rows(out_ref, third, rows[: eight * groups])
    extra.append(jnp.zeros_like(extra[0]))
    put_rows(out_ref, thirds, mul(spread_ref[...], jnp.concatenate(extra, axis=0)))


def multiply_kernel(in_ref, sort_ref, unsort_ref, blocks_ref, out_ref, sorted_ref):
    groups, thirds, _, states = in_ref.shape
    half = thirds * groups
    for third in range(thirds):
        rows = mul(sort_ref[...], rows_of(in_ref, third)).astype(jnp.bfloat16)
        for block in range(8):
            at = block * half + third * groups
            sorted_ref[at : at + groups] = rows[block * groups : (block + 1) * groups]

    def product(frequency, re_at, im_at, count):
        re = sorted_ref[re_at : re_at + count]
        im = sorted_ref[im_at : im_at + count]
        left = jnp.concatenate(
            [jnp.concatenate([re, -im], axis=1), jnp.concatenate([im, re], axis=1)], axis=0
        )
        right = jnp.concatenate([blocks_ref[0, frequency], blocks_ref[1, frequency]], axis=0)
        rows = mul(left, right).astype(jnp.bfloat16)
        sorted_ref[re_at : re_at + count] = rows[:count]
        sorted_ref[im_at : im_at + count] = rows[count:]

    product(1, 0, 2 * half, 2 * half)
    product(0, 4 * half, 6 * half, half)
    product(2, 5 * half, 7 * half, half)
    for third in range(thirds):
        at = third * groups
        rows = [sorted_ref[block * half + at : block * half + at + groups] for block in range(8)]
        put_rows(out_ref, third, mul(unsort_ref[...], jnp.concatenate(rows, axis=0)))


def carry_kernel(in_ref, objective_ref, jacobians_ref, pack_ref, unpack_ref, send_ref,
                 following_ref, sum_ref):
    steps, columns, states = objective_ref.shape
    thirds = in_ref.shape[1]
    width = columns // thirds
    for third in range(thirds):
        rows = mul(unpack_ref[...], rows_of(in_ref, third)).astype(jnp.bfloat16)
        following_ref[:, third * width : (third + 1) * width] = rows.reshape(steps, width, states)
    at_end = lax.axis_index("tm") == in_ref.shape[0] - 1
    for step in range(steps):
        carried = mul(following_ref[step], jacobians_ref[step])
        if step == steps - 1:
            carried = jnp.where(at_end, 0.0, 1.0) * carried
        sum_ref[step] = (objective_ref[step] + carried).astype(jnp.bfloat16)
    for third in range(thirds):
        rows = sum_ref[:, third * width : (third + 1) * width]
        put_rows(send_ref, third, mul(pack_ref[...], rows.reshape(steps * width, states)))


def finish_kernel(in_ref, objective_ref, jacobians_ref, unpack_ref, sort_ref,
                  adjoint_hbm, residual_hbm, adjoint_ref, residual_ref, sem):
    steps, columns, states = objective_ref.shape
    thirds = in_ref.shape[1] - 1
    width = columns // thirds
    copies = []

    def put(source, target, part, flag):
        copies.append(pltpu.make_async_copy(source.at[part], target.at[part], flag))
        copies[-1].start()

    for third in range(thirds):
        rows = mul(unpack_ref[...], rows_of(in_ref, third))
        adjoint_ref[:, third * width : (third + 1) * width] = rows.reshape(steps, width, states)
        part = (slice(None), pl.ds(third * width, width))
        put(adjoint_ref, adjoint_hbm, part, sem.at[0, third])
    for step in range(steps):
        if step + 1 < steps:
            following = adjoint_ref[step + 1].astype(jnp.bfloat16)
        else:
            following = mul(sort_ref[...], rows_of(in_ref, thirds))[:columns]
            following = following.astype(jnp.bfloat16)
        carried = mul(following, jacobians_ref[step])
        residual_ref[step] = objective_ref[step] - (adjoint_ref[step] - carried)
        put(residual_ref, residual_hbm, step, sem.at[1, step])
    for copy in copies:
        copy.wait()


def call(kernel, out_shape, args, limit, scratch=(), out_space=pltpu.VMEM, flops=1 << 28):
    return pl.pallas_call(
        kernel,
        out_shape=out_shape,
        in_specs=[pl.BlockSpec(memory_space=pltpu.VMEM)] * len(args),
        out_specs=jax.tree.map(lambda _: pl.BlockSpec(memory_space=out_space), out_shape),
        scratch_shapes=list(scratch),
        compiler_params=pltpu.CompilerParams(vmem_limit_bytes=limit * MIB),
        cost_estimate=pl.CostEstimate(flops=flops, bytes_accessed=4 * MIB, transcendentals=0),
    )(*args)


def exchange(block):
    return lax.all_to_all(block, "tm", split_axis=0, concat_axis=0, tiled=True)


def body(objective, jacobians, precond_blocks):
    local_steps, columns, states = objective.shape
    groups = lax.axis_size("tm")
    steps = local_steps * groups
    thirds = columns // (2 * groups)
    forward, backward, forward_next, backward_next, beyond = tables(steps, groups)
    both = np.concatenate([backward, beyond], axis=0)
    forward, second, both, backward_next = (
        split_table(t)
        for t in (
            forward,
            np.concatenate([forward, -forward_next], axis=1),
            np.concatenate([both, both], axis=1),
            backward_next,
        )
    )
    pack, sort = shuffles(groups)
    unpack, unsort = pack.T.copy(), sort.T.copy()
    forward, second, both, backward_next, pack, unpack, sort, unsort = (
        jnp.asarray(t)
        for t in (forward, second, both, backward_next, pack, unpack, sort, unsort)
    )
    wire = jax.ShapeDtypeStruct((groups, thirds, 8, states), jnp.bfloat16)
    longer = jax.ShapeDtypeStruct((groups, thirds + 1, 8, states), jnp.bfloat16)
    field = jax.ShapeDtypeStruct(objective.shape, jnp.float32)

    def multiply(rows):
        return call(
            multiply_kernel,
            wire,
            (rows, sort, unsort, precond_blocks),
            16,
            scratch=[pltpu.VMEM((4 * columns, states), jnp.bfloat16)],
            flops=1 << 31,
        )

    send = call(pack_kernel, wire, (objective,), 16)
    rows = call(transform_kernel, wire, (exchange(send), forward), 16)
    wave = exchange(multiply(exchange(rows)))
    ahead = call(transform_kernel, wire, (wave, backward_next), 16)
    send = call(
        carry_kernel,
        wire,
        (exchange(ahead), objective, jacobians, pack, unpack),
        16,
        scratch=[pltpu.VMEM(objective.shape, jnp.bfloat16)] * 2,
        flops=1 << 30,
    )
    rows = call(transform_kernel, wire, (exchange(send), ahead, second), 16)
    again = exchange(multiply(exchange(rows)))
    rows = call(last_transform_kernel, longer, (wave, again, both, unsort), 16)
    return call(
        finish_kernel,
        (field, field),
        (exchange(rows), objective, jacobians, unpack, sort),
        16,
        scratch=[
            pltpu.VMEM(objective.shape, jnp.float32),
            pltpu.VMEM(objective.shape, jnp.float32),
            pltpu.SemaphoreType.DMA((2, local_steps)),
        ],
        out_space=pl.ANY,
        flops=1 << 30,
    )


def solution(mesh):
    in_specs = (P("tm", "obj", None), P("tm", None, None), P(None, "tm", None, None))
    out_specs = (P("tm", "obj", None), P("tm", "obj", None))
    return jax.shard_map(body, mesh=mesh, in_specs=in_specs, out_specs=out_specs, check_vma=False)
```
